256 devices in a mesh: hyp: 4 (over y), row: 8 (over x, core), col: 8 (over z).
Axes of the slice: x: 4, y: 4, z: 8, core: 2. Of those that a mesh axis runs over, the one named last changes fastest.
Arguments:
- left_factors: bfloat16 [4, 48, 48, 256, 256], P('hyp', 'row', 'col'), may hold values from -0.0546875 to 0.0546875
- right_factors: bfloat16 [4, 48, 48, 256, 256], P('hyp', 'row', 'col'), may hold values from -0.375 to 0.375
- admissible: int32 [48, 48], P('row', 'col'), may hold values from 0 to 1, as said below
- tile_ranks: int32 [4, 48, 48], P('hyp', 'row', 'col'), may hold values from 32 to 256
- probes: bfloat16 [12288, 128], P('col', 'row'), may hold values from -6 to 6
- solved_probes: bfloat16 [12288, 128], P('row', 'col'), may hold values from -180 to 180
- data_terms: float32 [4], P('hyp'), may hold values from -64 to 64
- log_params: float32 [4], replicated, may hold values from -4 to 4
Outputs:
- forward: bfloat16 [4, 12288, 128], P('hyp', 'row', 'col')
- backward: bfloat16 [4, 12288, 128], P('hyp', 'col', 'row')
- new_params: float32 [4], replicated
The draws below stay inside these ranges and needn't reach their ends.
Inputs may be any that keep to these rules, and one draw needn't show every extreme that they name: `admissible`: Symmetric; diagonal tiles are near field (0); a tile is near field when it lies within a small drawn reach of the diagonal. `tile_ranks`: only read for far-field tiles.
All inputs are finite; a program needn't handle non-finite values.
Results may differ from the reference program's by a relative error of at most 0.0046.
The reference program's roundings to bfloat16 on the way count: a program that leaves them out, or rounds other values in their place, can miss the bound.
Values may be sent and summed in bfloat16 or wider, within the bound.
No kernel may reach another device: no remote copies, remote signals or barrier semaphores. Data moves between devices by JAX's collectives and lax.ppermute only.
A program may use at most 64 MiB of HBM per device.

```python
import jax
import jax.numpy as jnp
from jax import lax

B = 256
R = 256
P_SIZE = 128
NB = 48
DERIVS = 4
N = 12288


def draw_admissible(key, part):
    reach = jax.random.randint(jax.random.fold_in(key, 11), (NB,), 0, 3)
    index = jnp.arange(NB).astype(jnp.int32)
    apart = jnp.abs(index[:, None] - index[None, :])
    near = apart <= jnp.maximum(reach[:, None], reach[None, :])
    return jnp.where(near, 0, 1).astype(jnp.int32)


def draw_solved_probes(key, part):
    first = jax.random.fold_in(jax.random.fold_in(key, 23), 0)
    rows = jnp.arange(NB * B).astype(jnp.float32) / (NB * B)
    cols = jnp.arange(P_SIZE).astype(jnp.float32) / P_SIZE
    base = jnp.clip(jax.random.normal(first, (NB * B, P_SIZE), jnp.float32), -6.0, 6.0)
    col_scale = jnp.power(3.0, cols)
    row_scale = jnp.power(10.0, rows)
    return (base * row_scale[:, None] * col_scale[None, :]).astype(jnp.bfloat16)


def plant(drawn, key, least, top_value):
    longest = drawn.shape.index(max(drawn.shape))
    spots = []
    for shift in (0, 1):
        where = [jax.random.randint(jax.random.fold_in(key, axis), (), 0, length) for axis, length in enumerate(drawn.shape)]
        where[longest] = (where[longest] + shift) % drawn.shape[longest]
        spots.append(tuple(where))
    return drawn.at[spots[0]].set(least).at[spots[1]].set(top_value)


def block_scale(own_key, shape, cuts, smallest, high):
    factor_of, own = 1.0, jax.random.fold_in(own_key, 6)
    for dim, blocks in cuts:
        heights = jnp.exp(jax.random.uniform(jax.random.fold_in(own, dim), (blocks,), jnp.float32, smallest / len(cuts), high / len(cuts)))
        factor_of = factor_of * jnp.repeat(heights, shape[dim] // blocks).reshape([-1 if axis == dim else 1 for axis in range(len(shape))])
    return factor_of


def bell_draw(key, extent, scale, limit, shards=(), kind=jnp.bfloat16):
    drawn = jax.random.normal(key, extent, jnp.float32) * scale
    if len(shards) > 0:
        drawn = block_scale(key, extent, shards, -0.22, 0.18) * drawn
    return jnp.clip(drawn, min=-limit, max=limit).astype(kind)


def setup_inputs(seed: int = 0) -> dict:
    seeds = jax.random.split(jax.random.key(seed), 9)
    return {
        "left_factors": bell_draw(seeds[0], (DERIVS, NB, NB, B, R), (R * NB) ** -0.5, 0.0546875, ((0, 4), (1, 8), (2, 8))),
        "right_factors": bell_draw(seeds[1], (DERIVS, NB, NB, B, R), B ** -0.5, 0.375, ((0, 4), (1, 8), (2, 8))),
        "admissible": draw_admissible(jax.random.fold_in(seeds[8], 71), 0),
        "tile_ranks": plant(jax.random.randint(seeds[3], (DERIVS, NB, NB), R // 8, R + 1), jax.random.fold_in(seeds[3], 1), R // 8, R).astype(jnp.int32),
        "probes": bell_draw(seeds[4], (N, P_SIZE), 1.0, 6.0, ((0, 8), (1, 8))),
        "solved_probes": draw_solved_probes(jax.random.fold_in(seeds[8], 71), 0),
        "data_terms": bell_draw(seeds[6], (DERIVS,), 10.0, 64.0, ((0, 4),), jnp.float32),
        "log_params": bell_draw(seeds[7], (DERIVS,), 1.0, 4.0, (), jnp.float32),
    }


step_rate = 0.5

def tile_masks(admissible, ranks):
    used = jnp.where(admissible == 0, R, ranks).astype(jnp.int32)
    slots = jnp.arange(R).astype(jnp.int32)
    return (slots[None, None, :] < used[:, :, None]).astype(jnp.float32)

def rounded(values):
    return lax.optimization_barrier(values.astype(jnp.bfloat16)).astype(jnp.float32)

def reference(left_factors, right_factors, admissible, tile_ranks, probes, solved_probes, data_terms, log_params):
    probe_blocks = probes.astype(jnp.float32).reshape(NB, B, P_SIZE)
    solved_blocks = solved_probes.astype(jnp.float32).reshape(NB, B, P_SIZE)
    solved_full = solved_probes.astype(jnp.float32)

    def one_matrix(items):
        left_tiles, right_tiles, ranks = items
        kept = tile_masks(admissible, ranks)

        def block_row(parts):
            left_row, right_row, kept_row = parts
            coefs = jnp.einsum('jbr,jbp->jrp', right_row.astype(jnp.float32), probe_blocks) * kept_row[:, :, None]
            return jnp.einsum('jbr,jrp->bp', left_row.astype(jnp.float32), rounded(coefs))

        def block_col(parts):
            left_col, right_col, kept_col = parts
            coefs = jnp.einsum('ibr,ibp->irp', left_col.astype(jnp.float32), solved_blocks) * kept_col[:, :, None]
            return jnp.einsum('ibr,irp->bp', right_col.astype(jnp.float32), rounded(coefs))
        rows_out = lax.map(block_row, (left_tiles, right_tiles, kept))
        cols_out = lax.map(block_col, (jnp.swapaxes(left_tiles, 0, 1), jnp.swapaxes(right_tiles, 0, 1), jnp.swapaxes(kept, 0, 1)))
        forward_full = rows_out.reshape(NB * B, P_SIZE)
        trace_value = jnp.sum(solved_full * forward_full) / P_SIZE
        return (forward_full.astype(jnp.bfloat16), cols_out.reshape(NB * B, P_SIZE).astype(jnp.bfloat16), trace_value)
    forward, backward, traces = lax.map(one_matrix, (left_factors, right_factors, tile_ranks))
    gradient = 0.5 * (data_terms - traces)
    grad_norm = jnp.sqrt(jnp.sum(gradient * gradient))
    new_params = log_params - step_rate * gradient / grad_norm
    return (forward, backward, new_params)
```

```python
import jax
import jax.numpy as jnp
from jax import lax
from jax.experimental import pallas as pl
from jax.experimental.pallas import tpu as pltpu
from jax.sharding import Mesh
from jax.sharding import PartitionSpec as P

ROW = ("row_0", "row_1")
PLANE = ("hyp", "row_0", "row_1")
STEP_RATE = 0.5
LANES = 128
GROUP = 2


VMEM = pl.BlockSpec(memory_space=pltpu.VMEM)
SMEM = pl.BlockSpec(memory_space=pltpu.SMEM)
HBM = pl.BlockSpec(memory_space=pltpu.HBM)


def call(kernel, out_shape, in_specs, name, flops=0, scratch=(), out_specs=VMEM):
    return pl.pallas_call(
        kernel,
        out_shape=out_shape,
        in_specs=in_specs,
        out_specs=out_specs,
        scratch_shapes=scratch,
        name=name,
        cost_estimate=pl.CostEstimate(flops=flops, bytes_accessed=flops // 64, transcendentals=0),
        compiler_params=pltpu.CompilerParams(vmem_limit_bytes=24 * 1024 * 1024),
    )


def times_tile(rows, tile):
    return lax.dot_general(rows, tile, (((1,), (0,)), ((), ())), preferred_element_type=jnp.float32)


def times_tile_transposed(rows, tile):
    return lax.dot_general(rows, tile, (((1,), (1,)), ((), ())), preferred_element_type=jnp.float32)


def two_sided(wide, first, second, kept, outer, inner, tile_of, coefs, store, reads):
    height, leaf = wide.shape[0], first.shape[-1]

    def coef(o, n):
        i, j = tile_of(o, n)
        mask = kept[i * first.shape[1] + j : i * first.shape[1] + j + 1, :]
        values = times_tile(wide[:, leaf * n : leaf * (n + 1)], first[i, j])
        coefs[o % 2, :, leaf * n : leaf * (n + 1)] = (values * mask).astype(jnp.bfloat16)

    for start in range(0, outer, GROUP):
        group = range(start, min(start + GROUP, outer))
        for o in group:
            for read in reads[o]:
                read.wait()
        for n in range(inner):
            coef(start, n)
        for o in group:
            total = jnp.zeros((height, leaf), jnp.float32)
            for n in range(inner):
                if o + 1 in group:
                    coef(o + 1, n)
                i, j = tile_of(o, n)
                rows = coefs[o % 2, :, leaf * n : leaf * (n + 1)]
                total += times_tile_transposed(rows, second[i, j])
            store(o, total)


def panel_rows(k, height):
    return pl.ds(pl.multiple_of(height * lax.rem(k, 8), height), height)


def column_pieces(own, near, far):
    up_1, down_1, up_2, down_2 = near
    up_far, down_far = far
    length = own.shape[1]
    split = length // 2
    return (
        (0, 0, length, own, 0),
        (1, 0, length, up_1, 0),
        (7, 0, length, down_1, 0),
        (2, 0, length, up_2, 0),
        (6, 0, length, down_2, 0),
        (3, 0, length, up_far, 0),
        (5, 0, length, down_far, 0),
        (4, 0, split, up_far, length),
        (4, split, split, down_far, length),
    )


def relay_kernel(up_1, down_1, up_2, down_2, up, down):
    length = up_1.shape[1]
    split = length // 2
    up[:, :length] = up_1[...]
    up[:, length:] = up_2[:, :split]
    down[:, :length] = down_1[...]
    down[:, length:] = down_2[:, split:]


def forward_kernel(*refs):
    panels = refs[:8]
    admissible_hbm, ranks_hbm, left_hbm, right_hbm, out, kept = refs[8:14]
    left, right, wide, coefs, admissible, ranks, sems = refs[14:]
    n_i, n_j, leaf, cap = left.shape
    x, core = lax.axis_index("row_0"), lax.axis_index("row_1")
    height = panels[0].shape[0]

    def rows(k, h):
        return panel_rows(2 * (x + 4 - k) + lax.rem(core + h, 2), height)

    small = [
        pltpu.make_async_copy(admissible_hbm, admissible, sems.at[2 * n_i]),
        pltpu.make_async_copy(ranks_hbm, ranks, sems.at[2 * n_i + 1]),
        pltpu.make_async_copy(panels[0], wide.at[rows(0, 0)], sems.at[2 * n_i + 2]),
    ]
    reads = [
        [
            pltpu.make_async_copy(source.at[i], target.at[i], sems.at[2 * i + side])
            for side, (source, target) in enumerate(((right_hbm, right), (left_hbm, left)))
        ]
        for i in range(n_i)
    ]
    for read in small + sum(reads, []):
        read.start()
    for k in range(4):
        for h in range(2):
            if k or h:
                wide[rows(k, h), :] = panels[2 * k + h][...]
    for read in small:
        read.wait()
    slot = lax.broadcasted_iota(jnp.int32, (1, cap), 1)
    for i in range(n_i):
        for j in range(n_j):
            used = jnp.where(admissible[i, j] == 0, cap, ranks[i, 0, j])
            kept[i * n_j + j : i * n_j + j + 1, :] = (slot < used).astype(jnp.float32)

    def store(i, total):
        out[:, leaf * i : leaf * (i + 1)] = total

    two_sided(wide, right, left, kept, n_i, n_j, lambda i, j: (i, j), coefs, store, reads)


def backward_kernel(kept, own, *refs):
    near, far = refs[:4], refs[4:6]
    left_hbm, right_hbm, keep, give, left, right, wide, coefs, sems = refs[6:]
    n_i, n_j, leaf, _ = left.shape
    reads = [
        [
            pltpu.make_async_copy(source.at[:, j], target.at[:, j], sems.at[2 * j + side])
            for side, (source, target) in enumerate(((left_hbm, left), (right_hbm, right)))
        ]
        for j in range(n_j)
    ]
    for pair in reads:
        for read in pair:
            read.start()
    core, z = lax.axis_index("row_1"), lax.axis_index("col")
    height = keep.shape[1]
    for back, start, lanes, ref, at in column_pieces(own, near, far):
        wide[panel_rows(z + 8 - back, height), start : start + lanes] = ref[:, at : at + lanes]

    def store(j, total):
        where = slice(leaf * j, leaf * (j + 1))
        for x in range(4):
            first = total[2 * x * height : (2 * x + 1) * height]
            second = total[(2 * x + 1) * height : (2 * x + 2) * height]
            keep[x, :, where] = jnp.where(core == 0, first, second)
            give[x, :, where] = jnp.where(core == 0, second, first)

    two_sided(wide, left, right, kept, n_j, n_i, lambda j, i: (i, j), coefs, store, reads)


def message_kernel(forward, own, *refs):
    near, far, out = refs[:4], refs[4:6], refs[6]
    panels, height, width = out.shape
    length = width - LANES
    z = lax.axis_index("col")
    lane_sums = jnp.zeros((1, LANES), jnp.float32)
    for back, start, lanes, ref, at in column_pieces(own, near, far):
        panel = forward[panel_rows(z + 8 - back, height), start : start + lanes]
        panel *= ref[:, at : at + lanes].astype(jnp.float32)
        row_sums = jnp.sum(panel, axis=0, keepdims=True)
        for lane in range(0, lanes, LANES):
            lane_sums += row_sums[:, lane : lane + LANES]
    top = lane_sums.astype(jnp.bfloat16).astype(jnp.float32)
    middle = (lane_sums - top).astype(jnp.bfloat16).astype(jnp.float32)
    bottom = lane_sums - top - middle
    row = lax.broadcasted_iota(jnp.int32, (height, LANES), 0)
    tail = jnp.where(row == 0, top, jnp.where(row == 1, middle, jnp.where(row == 2, bottom, 0.0)))
    for p in range(panels):
        out[p, :, :length] = forward[height * p : height * (p + 1), :].astype(jnp.bfloat16)
        out[p, :, length:] = tail.astype(jnp.bfloat16)


def share_kernel(data_terms, received, shares):
    length = received.shape[2] - LANES
    tails = received[0, :, length:].astype(jnp.float32)
    for p in range(1, received.shape[0]):
        tails += received[p, :, length:].astype(jnp.float32)
    share = data_terms[0] / 8 - jnp.sum(tails) / LANES
    shares[...] = jnp.full(shares.shape, share, jnp.float32)


def forward_sum_kernel(received, out):
    length = out.shape[1]
    total = received[0, :, :length].astype(jnp.float32)
    for p in range(1, received.shape[0]):
        total += received[p, :, :length].astype(jnp.float32)
    out[...] = total.astype(jnp.bfloat16)


def core_sum_kernel(keep, taken, own, next_1, next_2, next_3):
    x = lax.axis_index("row_0")
    own[...] = keep[x] + taken[x]
    for k, out in ((1, next_1), (2, next_2), (3, next_3)):
        place = lax.rem(x + k, 4)
        out[...] = (keep[place] + taken[place]).astype(jnp.bfloat16)


def backward_sum_kernel(own, part_1, part_2, part_3, out):
    total = own[...] + part_1[...].astype(jnp.float32)
    total += part_2[...].astype(jnp.float32) + part_3[...].astype(jnp.float32)
    out[...] = total.astype(jnp.bfloat16)


def step_kernel(log_params, shares, out):
    derivs = log_params.shape[0]
    group = shares.shape[0] // derivs
    gradients = [
        0.5 * jnp.sum(shares[group * j : group * (j + 1), 0, :], axis=0, keepdims=True)
        for j in range(derivs)
    ]
    norm = jnp.sqrt(sum(g * g for g in gradients))
    lane = lax.broadcasted_iota(jnp.int32, (1, LANES), 1)
    stepped = jnp.zeros((1, LANES), jnp.float32)
    for j, g in enumerate(gradients):
        stepped = jnp.where(lane == j, log_params[j] - STEP_RATE * g / norm, stepped)
    out[...] = stepped[0, :derivs]


def in_hbm(array):
    return pltpu.with_memory_space_constraint(array, pltpu.HBM)


def rotated(array, axis, k):
    size = lax.axis_size(axis)
    return lax.ppermute(array, axis, [(i, (i + k) % size) for i in range(size)])


def local(left, right, admissible, ranks, probes, solved, data_terms, log_params):
    left, right = left[0], right[0]
    n_i, n_j, leaf, cap = left.shape
    ranks = ranks.reshape(n_i, 1, n_j)
    tile_flops = 2 * leaf * cap * 128
    bf16, f32 = jnp.bfloat16, jnp.float32
    own_s, own_x = solved.T, probes.T
    height, length = own_x.shape
    panels = 8
    wide_scratch = pltpu.VMEM((panels * height, length), bf16)
    factor_scratch = pltpu.VMEM(left.shape, bf16)
    coef_scratch = pltpu.VMEM((2, panels * height, length), bf16)

    with jax.named_scope("gather_x"):
        pieces = [own_x] + [None] * 3
        with jax.named_scope("hop"):
            for k in (1, 3, 2):
                pieces[k] = rotated(own_x, "row_0", k)
        with jax.named_scope("swap"):
            both = []
            for piece in pieces:
                both += [piece, rotated(piece, "row_1", 1)]

    with jax.named_scope("gather_s"):
        with jax.named_scope("near"):
            near = [rotated(own_s, "col", k) for k in (1, -1, 2, -2)]
        relayed = jax.ShapeDtypeStruct((height, length * 3 // 2), bf16)
        relays = call(
            relay_kernel,
            (relayed, relayed),
            [VMEM] * 4,
            "relay",
            flops=1024,
            out_specs=(VMEM, VMEM),
        )(*near)
        with jax.named_scope("far"):
            far = [rotated(piece, "col", k) for piece, k in zip(relays, (2, -2))]
        s_pieces = (own_s, *near, *far)

    with jax.named_scope("forward"):
        forward, kept = call(
            forward_kernel,
            (
                jax.ShapeDtypeStruct((panels * height, n_i * leaf), f32),
                jax.ShapeDtypeStruct((n_i * n_j, cap), f32),
            ),
            [HBM] + [VMEM] * 7 + [HBM] * 4,
            "forward",
            flops=2 * n_i * n_j * tile_flops,
            scratch=[factor_scratch] * 2
            + [
                wide_scratch,
                coef_scratch,
                pltpu.SMEM((n_i, n_j), jnp.int32),
                pltpu.SMEM((n_i, 1, n_j), jnp.int32),
                pltpu.SemaphoreType.DMA((2 * n_i + 3,)),
            ],
            out_specs=(VMEM, VMEM),
        )(in_hbm(own_x), *both[1:], *(in_hbm(a) for a in (admissible, ranks, left, right)))

    with jax.named_scope("message"):
        message = call(
            message_kernel,
            jax.ShapeDtypeStruct((panels, height, n_i * leaf + LANES), bf16),
            [VMEM] * 8,
            "message",
            flops=4 * panels * height * length,
        )(forward, *s_pieces)
    with jax.named_scope("scatter_f"):
        received = lax.all_to_all(message, "col", 0, 0, tiled=True)

    with jax.named_scope("backward"):
        piece_shape = jax.ShapeDtypeStruct((height, n_j * leaf), bf16)
        half = jax.ShapeDtypeStruct((4, height, n_j * leaf), f32)
        keep, give = call(
            backward_kernel,
            (half, half),
            [VMEM] * 8 + [HBM] * 2,
            "backward",
            flops=2 * n_i * n_j * tile_flops,
            out_specs=(VMEM, VMEM),
            scratch=[factor_scratch] * 2
            + [wide_scratch, coef_scratch, pltpu.SemaphoreType.DMA((2 * n_j,))],
        )(kept, *s_pieces, in_hbm(left), in_hbm(right))
        taken = rotated(give, "row_1", 1)
        own_b, *outgoing = call(
            core_sum_kernel,
            (jax.ShapeDtypeStruct((height, n_j * leaf), f32),) + (piece_shape,) * 3,
            [VMEM, VMEM],
            "core_sum",
            flops=4 * height * length,
            out_specs=(VMEM,) * 4,
        )(keep, taken)
        incoming = [rotated(outgoing[k - 1], "row_0", k) for k in (1, 3, 2)]
        backward_out = call(
            backward_sum_kernel, piece_shape, [VMEM] * 4, "backward_sum", flops=4 * height * length
        )(own_b, *incoming)

    with jax.named_scope("finish"):
        shares = call(
            share_kernel,
            jax.ShapeDtypeStruct((32, 1, LANES), f32),
            [SMEM, VMEM],
            "share",
            flops=8 * height * LANES,
        )(data_terms, received)
        all_shares = lax.all_to_all(shares, PLANE, 0, 0, tiled=True)
        forward_out = call(
            forward_sum_kernel, piece_shape, [VMEM], "forward_sum", flops=8 * height * length
        )(received)
        stepped = call(
            step_kernel,
            jax.ShapeDtypeStruct(log_params.shape, f32),
            [SMEM, VMEM],
            "step",
            flops=1024,
        )(log_params, all_shares)

    return forward_out.T[None], backward_out.T[None], stepped


def solution(mesh):
    finer = Mesh(
        mesh.devices.reshape(mesh.shape["hyp"], 4, 2, mesh.shape["col"]),
        ("hyp", "row_0", "row_1", "col"),
    )
    in_specs = (
        P("hyp", ROW, "col", None, None),
        P("hyp", ROW, "col", None, None),
        P(ROW, "col"),
        P("hyp", ROW, "col"),
        P("col", ROW),
        P(ROW, "col"),
        P("hyp"),
        P(),
    )
    out_specs = (P("hyp", ROW, "col"), P("hyp", "col", ROW), P())
    return jax.shard_map(
        local, mesh=finer, in_specs=in_specs, out_specs=out_specs, check_vma=False
    )
```

```python
import jax
import jax.numpy as jnp
from jax import lax
from jax.experimental import pallas as pl
from jax.experimental.pallas import tpu as pltpu
from jax.sharding import Mesh
from jax.sharding import PartitionSpec as P

ROW = ("row_0", "row_1")
PLANE = ("hyp", "row_0", "row_1")
STEP_RATE = 0.5
LANES = 128
GROUP = 2


VMEM = pl.BlockSpec(memory_space=pltpu.VMEM)
SMEM = pl.BlockSpec(memory_space=pltpu.SMEM)
HBM = pl.BlockSpec(memory_space=pltpu.HBM)


def call(kernel, out_shape, in_specs, flops=0, scratch=(), out_specs=VMEM):
    return pl.pallas_call(
        kernel,
        out_shape=out_shape,
        in_specs=in_specs,
        out_specs=out_specs,
        scratch_shapes=scratch,
        cost_estimate=pl.CostEstimate(flops=flops, bytes_accessed=flops // 64, transcendentals=0),
        compiler_params=pltpu.CompilerParams(vmem_limit_bytes=24 * 1024 * 1024),
    )


def times_tile(rows, tile):
    return lax.dot_general(rows, tile, (((1,), (0,)), ((), ())), preferred_element_type=jnp.float32)


def times_tile_transposed(rows, tile):
    return lax.dot_general(rows, tile, (((1,), (1,)), ((), ())), preferred_element_type=jnp.float32)


def two_sided(wide, first, second, kept, outer, inner, tile_of, coefs, store, reads):
    height, leaf = wide.shape[0], first.shape[-1]

    def coef(o, n):
        i, j = tile_of(o, n)
        mask = kept[i * first.shape[1] + j : i * first.shape[1] + j + 1, :]
        values = times_tile(wide[:, leaf * n : leaf * (n + 1)], first[i, j])
        coefs[o % 2, :, leaf * n : leaf * (n + 1)] = (values * mask).astype(jnp.bfloat16)

    for start in range(0, outer, GROUP):
        group = range(start, min(start + GROUP, outer))
        for o in group:
            for read in reads[o]:
                read.wait()
        for n in range(inner):
            coef(start, n)
        for o in group:
            total = jnp.zeros((height, leaf), jnp.float32)
            for n in range(inner):
                if o + 1 in group:
                    coef(o + 1, n)
                i, j = tile_of(o, n)
                rows = coefs[o % 2, :, leaf * n : leaf * (n + 1)]
                total += times_tile_transposed(rows, second[i, j])
            store(o, total)


def panel_rows(k, height):
    return pl.ds(pl.multiple_of(height * lax.rem(k, 8), height), height)


def column_pieces(own, near, far):
    up_1, down_1, up_2, down_2 = near
    up_far, down_far = far
    length = own.shape[1]
    split = length // 2
    return (
        (0, 0, length, own, 0),
        (1, 0, length, up_1, 0),
        (7, 0, length, down_1, 0),
        (2, 0, length, up_2, 0),
        (6, 0, length, down_2, 0),
        (3, 0, length, up_far, 0),
        (5, 0, length, down_far, 0),
        (4, 0, split, up_far, length),
        (4, split, split, down_far, length),
    )


def stack_kernel(*refs):
    height = refs[0].shape[0]
    for k, ref in enumerate(refs[:-1]):
        refs[-1][height * k : height * (k + 1), :] = ref[...]


def relay_kernel(up_1, down_1, up_2, down_2, up, down):
    length = up_1.shape[1]
    split = length // 2
    up[:, :length] = up_1[...]
    up[:, length:] = up_2[:, :split]
    down[:, :length] = down_1[...]
    down[:, length:] = down_2[:, split:]


def forward_kernel(*refs):
    own, other, hops, other_hops = refs[:4]
    admissible_hbm, ranks_hbm, left_hbm, right_hbm, out, kept = refs[4:10]
    left, right, wide, coefs, admissible, ranks, sems = refs[10:]
    n_i, n_j, leaf, cap = left.shape
    x, core = lax.axis_index("row_0"), lax.axis_index("row_1")
    height = own.shape[0]

    def rows(k, h):
        return panel_rows(2 * (x + 4 - k) + lax.rem(core + h, 2), height)

    small = [
        pltpu.make_async_copy(admissible_hbm, admissible, sems.at[2 * n_i]),
        pltpu.make_async_copy(ranks_hbm, ranks, sems.at[2 * n_i + 1]),
        pltpu.make_async_copy(own, wide.at[rows(0, 0)], sems.at[2 * n_i + 2]),
    ]
    reads = [
        [
            pltpu.make_async_copy(source.at[i], target.at[i], sems.at[2 * i + side])
            for side, (source, target) in enumerate(((right_hbm, right), (left_hbm, left)))
        ]
        for i in range(n_i)
    ]
    for read in small + sum(reads, []):
        read.start()
    wide[rows(0, 1), :] = other[...]
    for k in range(1, 4):
        part = slice(height * (k - 1), height * k)
        wide[rows(k, 0), :] = hops[part, :]
        wide[rows(k, 1), :] = other_hops[part, :]
    for read in small:
        read.wait()
    slot = lax.broadcasted_iota(jnp.int32, (1, cap), 1)
    for i in range(n_i):
        for j in range(n_j):
            used = jnp.where(admissible[i, j] == 0, cap, ranks[i, 0, j])
            kept[i * n_j + j : i * n_j + j + 1, :] = (slot < used).astype(jnp.float32)

    def store(i, total):
        out[:, leaf * i : leaf * (i + 1)] = total

    two_sided(wide, right, left, kept, n_i, n_j, lambda i, j: (i, j), coefs, store, reads)


def backward_kernel(kept, own, *refs):
    near, far = refs[:4], refs[4:6]
    left_hbm, right_hbm, keep, give, left, right, wide, coefs, sems = refs[6:]
    n_i, n_j, leaf, _ = left.shape
    reads = [
        [
            pltpu.make_async_copy(source.at[:, j], target.at[:, j], sems.at[2 * j + side])
            for side, (source, target) in enumerate(((left_hbm, left), (right_hbm, right)))
        ]
        for j in range(n_j)
    ]
    for pair in reads:
        for read in pair:
            read.start()
    core, z = lax.axis_index("row_1"), lax.axis_index("col")
    height = keep.shape[1]
    for back, start, lanes, ref, at in column_pieces(own, near, far):
        wide[panel_rows(z + 8 - back, height), start : start + lanes] = ref[:, at : at + lanes]

    def store(j, total):
        where = slice(leaf * j, leaf * (j + 1))
        for x in range(4):
            first = total[2 * x * height : (2 * x + 1) * height]
            second = total[(2 * x + 1) * height : (2 * x + 2) * height]
            keep[x, :, where] = jnp.where(core == 0, first, second)
            give[x, :, where] = jnp.where(core == 0, second, first)

    two_sided(wide, left, right, kept, n_j, n_i, lambda j, i: (i, j), coefs, store, reads)


def message_kernel(forward, own, *refs):
    near, far, out = refs[:4], refs[4:6], refs[6]
    panels, height, width = out.shape
    length = width - LANES
    z = lax.axis_index("col")
    lane_sums = jnp.zeros((1, LANES), jnp.float32)
    for back, start, lanes, ref, at in column_pieces(own, near, far):
        panel = forward[panel_rows(z + 8 - back, height), start : start + lanes]
        panel *= ref[:, at : at + lanes].astype(jnp.float32)
        row_sums = jnp.sum(panel, axis=0, keepdims=True)
        for lane in range(0, lanes, LANES):
            lane_sums += row_sums[:, lane : lane + LANES]
    top = lane_sums.astype(jnp.bfloat16).astype(jnp.float32)
    middle = (lane_sums - top).astype(jnp.bfloat16).astype(jnp.float32)
    bottom = lane_sums - top - middle
    row = lax.broadcasted_iota(jnp.int32, (height, LANES), 0)
    tail = jnp.where(row == 0, top, jnp.where(row == 1, middle, jnp.where(row == 2, bottom, 0.0)))
    for p in range(panels):
        out[p, :, :length] = forward[height * p : height * (p + 1), :].astype(jnp.bfloat16)
        out[p, :, length:] = tail.astype(jnp.bfloat16)


def share_kernel(data_terms, received, shares):
    length = received.shape[2] - LANES
    tails = received[0, :, length:].astype(jnp.float32)
    for p in range(1, received.shape[0]):
        tails += received[p, :, length:].astype(jnp.float32)
    share = data_terms[0] / 8 - jnp.sum(tails) / LANES
    shares[...] = jnp.full(shares.shape, share, jnp.float32)


def forward_sum_kernel(received, out):
    length = out.shape[1]
    total = received[0, :, :length].astype(jnp.float32)
    for p in range(1, received.shape[0]):
        total += received[p, :, :length].astype(jnp.float32)
    out[...] = total.astype(jnp.bfloat16)


def core_sum_kernel(keep, taken, own, next_1, next_2, next_3):
    x = lax.axis_index("row_0")
    own[...] = keep[x] + taken[x]
    for k, out in ((1, next_1), (2, next_2), (3, next_3)):
        place = lax.rem(x + k, 4)
        out[...] = (keep[place] + taken[place]).astype(jnp.bfloat16)


def backward_sum_kernel(own, part_1, part_2, part_3, out):
    total = own[...] + part_1[...].astype(jnp.float32)
    total += part_2[...].astype(jnp.float32) + part_3[...].astype(jnp.float32)
    out[...] = total.astype(jnp.bfloat16)


def step_kernel(log_params, shares, out):
    derivs = log_params.shape[0]
    group = shares.shape[0] // derivs
    gradients = [
        0.5 * jnp.sum(shares[group * j : group * (j + 1), 0, :], axis=0, keepdims=True)
        for j in range(derivs)
    ]
    norm = jnp.sqrt(sum(g * g for g in gradients))
    lane = lax.broadcasted_iota(jnp.int32, (1, LANES), 1)
    change = jnp.zeros((1, LANES), jnp.float32)
    for j, g in enumerate(gradients):
        change = jnp.where(lane == j, STEP_RATE * g / norm, change)
    out[...] = log_params[...] - change[0, :derivs]


def in_hbm(array):
    return pltpu.with_memory_space_constraint(array, pltpu.HBM)


def rotated(array, axis, k):
    size = lax.axis_size(axis)
    return lax.ppermute(array, axis, [(i, (i + k) % size) for i in range(size)])


def local(left, right, admissible, ranks, probes, solved, data_terms, log_params):
    left, right = left[0], right[0]
    n_i, n_j, leaf, cap = left.shape
    ranks = ranks.reshape(n_i, 1, n_j)
    tile_flops = 2 * leaf * cap * 128
    bf16, f32 = jnp.bfloat16, jnp.float32
    own_s, own_x = solved.T, probes.T
    height, length = own_x.shape
    panels = 8
    wide_scratch = pltpu.VMEM((panels * height, length), bf16)
    factor_scratch = pltpu.VMEM(left.shape, bf16)
    coef_scratch = pltpu.VMEM((2, panels * height, length), bf16)

    pieces = [own_x] + [None] * 3
    for k in (1, 3, 2):
        pieces[k] = rotated(own_x, "row_0", k)
    other_x = rotated(own_x, "row_1", 1)
    stacked = call(
        stack_kernel, jax.ShapeDtypeStruct((3 * height, length), bf16), [VMEM] * 3, flops=1024
    )(*pieces[1:])
    other_stacked = rotated(stacked, "row_1", 1)
    both = [own_x, other_x, stacked, other_stacked]

    near = []
    for k in (1, -1, 2, -2):
        near.append(rotated(own_s, "col", k))
    relayed = jax.ShapeDtypeStruct((height, length * 3 // 2), bf16)
    relays = call(
        relay_kernel, (relayed, relayed), [VMEM] * 4, flops=1024, out_specs=(VMEM, VMEM)
    )(*near)
    far = [rotated(piece, "col", k) for piece, k in zip(relays, (2, -2))]
    s_pieces = (own_s, *near, *far)

    forward, kept = call(
        forward_kernel,
        (
            jax.ShapeDtypeStruct((panels * height, n_i * leaf), f32),
            jax.ShapeDtypeStruct((n_i * n_j, cap), f32),
        ),
        [HBM] + [VMEM] * 3 + [HBM] * 4,
        flops=2 * n_i * n_j * tile_flops,
        scratch=[factor_scratch] * 2
        + [
            wide_scratch,
            coef_scratch,
            pltpu.SMEM((n_i, n_j), jnp.int32),
            pltpu.SMEM((n_i, 1, n_j), jnp.int32),
            pltpu.SemaphoreType.DMA((2 * n_i + 3,)),
        ],
        out_specs=(VMEM, VMEM),
    )(in_hbm(own_x), *both[1:], *(in_hbm(a) for a in (admissible, ranks, left, right)))

    message = call(
        message_kernel,
        jax.ShapeDtypeStruct((panels, height, n_i * leaf + LANES), bf16),
        [VMEM] * 8,
        flops=4 * panels * height * length,
    )(forward, *s_pieces)
    received = lax.all_to_all(message, "col", 0, 0, tiled=True)

    piece_shape = jax.ShapeDtypeStruct((height, n_j * leaf), bf16)
    half = jax.ShapeDtypeStruct((4, height, n_j * leaf), f32)
    keep, give = call(
        backward_kernel,
        (half, half),
        [VMEM] * 8 + [HBM] * 2,
        flops=2 * n_i * n_j * tile_flops,
        out_specs=(VMEM, VMEM),
        scratch=[factor_scratch] * 2
        + [wide_scratch, coef_scratch, pltpu.SemaphoreType.DMA((2 * n_j,))],
    )(kept, *s_pieces, in_hbm(left), in_hbm(right))
    taken = rotated(give, "row_1", 1)
    own_b, *outgoing = call(
        core_sum_kernel,
        (jax.ShapeDtypeStruct((height, n_j * leaf), f32),) + (piece_shape,) * 3,
        [VMEM, VMEM],
        flops=4 * height * length,
        out_specs=(VMEM,) * 4,
    )(keep, taken)
    part_2 = rotated(outgoing[1], "row_0", 2)
    part_1, part_3 = (rotated(outgoing[k - 1], "row_0", k) for k in (1, 3))
    backward_out = call(
        backward_sum_kernel, piece_shape, [VMEM] * 4, flops=4 * height * length
    )(own_b, part_1, part_2, part_3)

    shares = call(
        share_kernel,
        jax.ShapeDtypeStruct((32, 1, LANES), f32),
        [SMEM, VMEM],
        flops=8 * height * LANES,
    )(data_terms, received)
    all_shares = lax.all_to_all(shares, PLANE, 0, 0, tiled=True)
    forward_out = call(forward_sum_kernel, piece_shape, [VMEM], flops=8 * height * length)(received)
    stepped = call(
        step_kernel, jax.ShapeDtypeStruct(log_params.shape, f32), [VMEM, VMEM], flops=1024
    )(log_params, all_shares)

    return forward_out.T[None], backward_out.T[None], stepped


def solution(mesh):
    finer = Mesh(
        mesh.devices.reshape(mesh.shape["hyp"], 4, 2, mesh.shape["col"]),
        ("hyp", "row_0", "row_1", "col"),
    )
    in_specs = (
        P("hyp", ROW, "col", None, None),
        P("hyp", ROW, "col", None, None),
        P(ROW, "col"),
        P("hyp", ROW, "col"),
        P("col", ROW),
        P(ROW, "col"),
        P("hyp"),
        P(),
    )
    out_specs = (P("hyp", ROW, "col"), P("hyp", "col", ROW), P())
    return jax.shard_map(local, mesh=finer, in_specs=in_specs, out_specs=out_specs, check_vma=False)
```

```python
import jax
import jax.numpy as jnp
from jax import lax
from jax.experimental import pallas as pl
from jax.experimental.pallas import tpu as pltpu
from jax.sharding import Mesh
from jax.sharding import PartitionSpec as P

ROW = ("row_0", "row_1")
PLANE = ("hyp", "row_0", "row_1")
STEP_RATE = 0.5
LANES = 128
GROUP = 2


VMEM = pl.BlockSpec(memory_space=pltpu.VMEM)
SMEM = pl.BlockSpec(memory_space=pltpu.SMEM)
HBM = pl.BlockSpec(memory_space=pltpu.HBM)


def call(kernel, out_shape, in_specs, name, flops=0, scratch=(), out_specs=VMEM):
    return pl.pallas_call(
        kernel,
        out_shape=out_shape,
        in_specs=in_specs,
        out_specs=out_specs,
        scratch_shapes=scratch,
        name=name,
        cost_estimate=pl.CostEstimate(flops=flops, bytes_accessed=flops // 64, transcendentals=0),
        compiler_params=pltpu.CompilerParams(vmem_limit_bytes=24 * 1024 * 1024),
    )


def times_tile(rows, tile):
    return lax.dot_general(rows, tile, (((1,), (0,)), ((), ())), preferred_element_type=jnp.float32)


def times_tile_transposed(rows, tile):
    return lax.dot_general(rows, tile, (((1,), (1,)), ((), ())), preferred_element_type=jnp.float32)


def two_sided(wide, first, second, kept, outer, inner, tile_of, coefs, store, reads):
    height, leaf = wide.shape[0], first.shape[-1]

    def coef(o, n):
        i, j = tile_of(o, n)
        mask = kept[i * first.shape[1] + j : i * first.shape[1] + j + 1, :]
        values = times_tile(wide[:, leaf * n : leaf * (n + 1)], first[i, j])
        coefs[o % 2, :, leaf * n : leaf * (n + 1)] = (values * mask).astype(jnp.bfloat16)

    for start in range(0, outer, GROUP):
        group = range(start, min(start + GROUP, outer))
        for o in group:
            for read in reads[o]:
                read.wait()
        for n in range(inner):
            coef(start, n)
        for o in group:
            total = jnp.zeros((height, leaf), jnp.float32)
            for n in range(inner):
                if o + 1 in group:
                    coef(o + 1, n)
                i, j = tile_of(o, n)
                rows = coefs[o % 2, :, leaf * n : leaf * (n + 1)]
                total += times_tile_transposed(rows, second[i, j])
            store(o, total)


def panel_rows(k, height):
    return pl.ds(pl.multiple_of(height * lax.rem(k, 8), height), height)


def column_pieces(own, near, far):
    up_1, down_1, up_2, down_2 = near
    up_far, down_far = far
    length = own.shape[1]
    split = length // 2
    return (
        (0, 0, length, own, 0),
        (1, 0, length, up_1, 0),
        (7, 0, length, down_1, 0),
        (2, 0, length, up_2, 0),
        (6, 0, length, down_2, 0),
        (3, 0, length, up_far, 0),
        (5, 0, length, down_far, 0),
        (4, 0, split, up_far, length),
        (4, split, split, down_far, length),
    )


def relay_kernel(up_1, down_1, up_2, down_2, up, down):
    length = up_1.shape[1]
    split = length // 2
    up[:, :length] = up_1[...]
    up[:, length:] = up_2[:, :split]
    down[:, :length] = down_1[...]
    down[:, length:] = down_2[:, split:]


def forward_kernel(*refs):
    panels = refs[:8]
    admissible_hbm, ranks_hbm, left_hbm, right_hbm, out, kept = refs[8:14]
    left, right, wide, coefs, admissible, ranks, sems = refs[14:]
    n_i, n_j, leaf, cap = left.shape
    x, core = lax.axis_index("row_0"), lax.axis_index("row_1")
    height = panels[0].shape[0]

    def rows(k, h):
        return panel_rows(2 * (x + 4 - k) + lax.rem(core + h, 2), height)

    small = [
        pltpu.make_async_copy(admissible_hbm, admissible, sems.at[2 * n_i]),
        pltpu.make_async_copy(ranks_hbm, ranks, sems.at[2 * n_i + 1]),
        pltpu.make_async_copy(panels[0], wide.at[rows(0, 0)], sems.at[2 * n_i + 2]),
    ]
    reads = [
        [
            pltpu.make_async_copy(source.at[i], target.at[i], sems.at[2 * i + side])
            for side, (source, target) in enumerate(((right_hbm, right), (left_hbm, left)))
        ]
        for i in range(n_i)
    ]
    for read in small + sum(reads, []):
        read.start()
    for k in range(4):
        for h in range(2):
            if k or h:
                wide[rows(k, h), :] = panels[2 * k + h][...]
    for read in small:
        read.wait()
    slot = lax.broadcasted_iota(jnp.int32, (1, cap), 1)
    for i in range(n_i):
        for j in range(n_j):
            used = jnp.where(admissible[i, j] == 0, cap, ranks[i, 0, j])
            kept[i * n_j + j : i * n_j + j + 1, :] = (slot < used).astype(jnp.float32)

    def store(i, total):
        out[:, leaf * i : leaf * (i + 1)] = total

    two_sided(wide, right, left, kept, n_i, n_j, lambda i, j: (i, j), coefs, store, reads)


def backward_kernel(kept, own, *refs):
    near, far = refs[:4], refs[4:6]
    left_hbm, right_hbm, keep, give, left, right, wide, coefs, sems = refs[6:]
    n_i, n_j, leaf, _ = left.shape
    reads = [
        [
            pltpu.make_async_copy(source.at[:, j], target.at[:, j], sems.at[2 * j + side])
            for side, (source, target) in enumerate(((left_hbm, left), (right_hbm, right)))
        ]
        for j in range(n_j)
    ]
    for pair in reads:
        for read in pair:
            read.start()
    core, z = lax.axis_index("row_1"), lax.axis_index("col")
    height = keep.shape[1]
    for back, start, lanes, ref, at in column_pieces(own, near, far):
        wide[panel_rows(z + 8 - back, height), start : start + lanes] = ref[:, at : at + lanes]

    def store(j, total):
        where = slice(leaf * j, leaf * (j + 1))
        for x in range(4):
            first = total[2 * x * height : (2 * x + 1) * height]
            second = total[(2 * x + 1) * height : (2 * x + 2) * height]
            keep[x, :, where] = jnp.where(core == 0, first, second)
            give[x, :, where] = jnp.where(core == 0, second, first)

    two_sided(wide, left, right, kept, n_j, n_i, lambda j, i: (i, j), coefs, store, reads)


def message_kernel(forward, own, *refs):
    near, far, out = refs[:4], refs[4:6], refs[6]
    panels, height, width = out.shape
    length = width - LANES
    z = lax.axis_index("col")
    lane_sums = jnp.zeros((1, LANES), jnp.float32)
    for back, start, lanes, ref, at in column_pieces(own, near, far):
        panel = forward[panel_rows(z + 8 - back, height), start : start + lanes]
        panel *= ref[:, at : at + lanes].astype(jnp.float32)
        row_sums = jnp.sum(panel, axis=0, keepdims=True)
        for lane in range(0, lanes, LANES):
            lane_sums += row_sums[:, lane : lane + LANES]
    top = lane_sums.astype(jnp.bfloat16).astype(jnp.float32)
    middle = (lane_sums - top).astype(jnp.bfloat16).astype(jnp.float32)
    bottom = lane_sums - top - middle
    row = lax.broadcasted_iota(jnp.int32, (height, LANES), 0)
    tail = jnp.where(row == 0, top, jnp.where(row == 1, middle, jnp.where(row == 2, bottom, 0.0)))
    for p in range(panels):
        out[p, :, :length] = forward[height * p : height * (p + 1), :].astype(jnp.bfloat16)
        out[p, :, length:] = tail.astype(jnp.bfloat16)


def share_kernel(data_terms, received, shares):
    length = received.shape[2] - LANES
    tails = received[0, :, length:].astype(jnp.float32)
    for p in range(1, received.shape[0]):
        tails += received[p, :, length:].astype(jnp.float32)
    share = data_terms[0] / 8 - jnp.sum(tails) / LANES
    shares[...] = jnp.full(shares.shape, share, jnp.float32)


def forward_sum_kernel(received, out):
    length = out.shape[1]
    total = received[0, :, :length].astype(jnp.float32)
    for p in range(1, received.shape[0]):
        total += received[p, :, :length].astype(jnp.float32)
    out[...] = total.astype(jnp.bfloat16)


def core_sum_kernel(keep, taken, own, next_1, next_2, next_3):
    x = lax.axis_index("row_0")
    own[...] = keep[x] + taken[x]
    for k, out in ((1, next_1), (2, next_2), (3, next_3)):
        place = lax.rem(x + k, 4)
        out[...] = (keep[place] + taken[place]).astype(jnp.bfloat16)


def backward_sum_kernel(own, part_1, part_2, part_3, out):
    total = own[...] + part_1[...].astype(jnp.float32)
    total += part_2[...].astype(jnp.float32) + part_3[...].astype(jnp.float32)
    out[...] = total.astype(jnp.bfloat16)


def step_kernel(log_params, shares, out):
    derivs = log_params.shape[0]
    group = shares.shape[0] // derivs
    gradients = [
        0.5 * jnp.sum(shares[group * j : group * (j + 1), 0, :], axis=0, keepdims=True)
        for j in range(derivs)
    ]
    norm = jnp.sqrt(sum(g * g for g in gradients))
    lane = lax.broadcasted_iota(jnp.int32, (1, LANES), 1)
    change = jnp.zeros((1, LANES), jnp.float32)
    for j, g in enumerate(gradients):
        change = jnp.where(lane == j, STEP_RATE * g / norm, change)
    out[...] = log_params[...] - change[0, :derivs]


def in_hbm(array):
    return pltpu.with_memory_space_constraint(array, pltpu.HBM)


def rotated(array, axis, k):
    size = lax.axis_size(axis)
    return lax.ppermute(array, axis, [(i, (i + k) % size) for i in range(size)])


def local(left, right, admissible, ranks, probes, solved, data_terms, log_params):
    left, right = left[0], right[0]
    n_i, n_j, leaf, cap = left.shape
    ranks = ranks.reshape(n_i, 1, n_j)
    tile_flops = 2 * leaf * cap * 128
    bf16, f32 = jnp.bfloat16, jnp.float32
    own_s, own_x = solved.T, probes.T
    height, length = own_x.shape
    panels = 8
    wide_scratch = pltpu.VMEM((panels * height, length), bf16)
    factor_scratch = pltpu.VMEM(left.shape, bf16)
    coef_scratch = pltpu.VMEM((2, panels * height, length), bf16)

    with jax.named_scope("gather_x"):
        pieces = [own_x] + [None] * 3
        with jax.named_scope("hop"):
            for k in (1, 3, 2):
                pieces[k] = rotated(own_x, "row_0", k)
        with jax.named_scope("swap"):
            both = []
            for piece in pieces:
                both += [piece, rotated(piece, "row_1", 1)]

    with jax.named_scope("gather_s"):
        with jax.named_scope("near"):
            near = [rotated(own_s, "col", k) for k in (1, -1, 2, -2)]
        relayed = jax.ShapeDtypeStruct((height, length * 3 // 2), bf16)
        relays = call(
            relay_kernel,
            (relayed, relayed),
            [VMEM] * 4,
            "relay",
            flops=1024,
            out_specs=(VMEM, VMEM),
        )(*near)
        with jax.named_scope("far"):
            far = [rotated(piece, "col", k) for piece, k in zip(relays, (2, -2))]
        s_pieces = (own_s, *near, *far)

    with jax.named_scope("forward"):
        forward, kept = call(
            forward_kernel,
            (
                jax.ShapeDtypeStruct((panels * height, n_i * leaf), f32),
                jax.ShapeDtypeStruct((n_i * n_j, cap), f32),
            ),
            [HBM] + [VMEM] * 7 + [HBM] * 4,
            "forward",
            flops=2 * n_i * n_j * tile_flops,
            scratch=[factor_scratch] * 2
            + [
                wide_scratch,
                coef_scratch,
                pltpu.SMEM((n_i, n_j), jnp.int32),
                pltpu.SMEM((n_i, 1, n_j), jnp.int32),
                pltpu.SemaphoreType.DMA((2 * n_i + 3,)),
            ],
            out_specs=(VMEM, VMEM),
        )(in_hbm(own_x), *both[1:], *(in_hbm(a) for a in (admissible, ranks, left, right)))

    with jax.named_scope("message"):
        message = call(
            message_kernel,
            jax.ShapeDtypeStruct((panels, height, n_i * leaf + LANES), bf16),
            [VMEM] * 8,
            "message",
            flops=4 * panels * height * length,
        )(forward, *s_pieces)
    with jax.named_scope("scatter_f"):
        received = lax.all_to_all(message, "col", 0, 0, tiled=True)

    with jax.named_scope("backward"):
        piece_shape = jax.ShapeDtypeStruct((height, n_j * leaf), bf16)
        half = jax.ShapeDtypeStruct((4, height, n_j * leaf), f32)
        keep, give = call(
            backward_kernel,
            (half, half),
            [VMEM] * 8 + [HBM] * 2,
            "backward",
            flops=2 * n_i * n_j * tile_flops,
            out_specs=(VMEM, VMEM),
            scratch=[factor_scratch] * 2
            + [wide_scratch, coef_scratch, pltpu.SemaphoreType.DMA((2 * n_j,))],
        )(kept, *s_pieces, in_hbm(left), in_hbm(right))
        taken = rotated(give, "row_1", 1)
        own_b, *outgoing = call(
            core_sum_kernel,
            (jax.ShapeDtypeStruct((height, n_j * leaf), f32),) + (piece_shape,) * 3,
            [VMEM, VMEM],
            "core_sum",
            flops=4 * height * length,
            out_specs=(VMEM,) * 4,
        )(keep, taken)
        incoming = [rotated(outgoing[k - 1], "row_0", k) for k in (1, 3, 2)]
        backward_out = call(
            backward_sum_kernel, piece_shape, [VMEM] * 4, "backward_sum", flops=4 * height * length
        )(own_b, *incoming)

    with jax.named_scope("finish"):
        shares = call(
            share_kernel,
            jax.ShapeDtypeStruct((32, 1, LANES), f32),
            [SMEM, VMEM],
            "share",
            flops=8 * height * LANES,
        )(data_terms, received)
        all_shares = lax.all_to_all(shares, PLANE, 0, 0, tiled=True)
        forward_out = call(
            forward_sum_kernel, piece_shape, [VMEM], "forward_sum", flops=8 * height * length
        )(received)
        stepped = call(
            step_kernel,
            jax.ShapeDtypeStruct(log_params.shape, f32),
            [VMEM, VMEM],
            "step",
            flops=1024,
        )(log_params, all_shares)

    return forward_out.T[None], backward_out.T[None], stepped


def solution(mesh):
    finer = Mesh(
        mesh.devices.reshape(mesh.shape["hyp"], 4, 2, mesh.shape["col"]),
        ("hyp", "row_0", "row_1", "col"),
    )
    in_specs = (
        P("hyp", ROW, "col", None, None),
        P("hyp", ROW, "col", None, None),
        P(ROW, "col"),
        P("hyp", ROW, "col"),
        P("col", ROW),
        P(ROW, "col"),
        P("hyp"),
        P(),
    )
    out_specs = (P("hyp", ROW, "col"), P("hyp", "col", ROW), P())
    return jax.shard_map(
        local, mesh=finer, in_specs=in_specs, out_specs=out_specs, check_vma=False
    )
```
